32 devices in a mesh: section: 2 (over core), tp: 4 (over y, x), fsdp: 4 (over z).
Axes of the slice: x: 2, y: 2, z: 4, core: 2. Of those that a mesh axis runs over, the one named last changes fastest.
Arguments:
- normed: bfloat16 [2, 256, 4608], P('section', 'tp', 'fsdp'), may hold values from -6 to 6
- cotangent: bfloat16 [2, 256, 4608], P('section', 'tp', 'fsdp'), may hold values from -6 to 6
- w_gate: bfloat16 [2, 4608, 18432], P('section', 'fsdp', 'tp'), may hold values from -0.09375 to 0.09375
- w_up: bfloat16 [2, 4608, 18432], P('section', 'fsdp', 'tp'), may hold values from -0.09375 to 0.09375
- w_down: bfloat16 [2, 4608, 18432], P('section', 'fsdp', 'tp'), may hold values from -0.046875 to 0.046875
Outputs:
- passed: bfloat16 [2, 256, 4608], P('section', 'tp', 'fsdp')
- grad_gate: bfloat16 [2, 4608, 18432], P('section', 'fsdp', 'tp')
- grad_up: bfloat16 [2, 4608, 18432], P('section', 'fsdp', 'tp')
- grad_down: bfloat16 [2, 4608, 18432], P('section', 'fsdp', 'tp')
The draws below stay inside these ranges and needn't reach their ends.
All inputs are finite; a program needn't handle non-finite values.
Results may differ from the reference program's by a relative error of at most 0.012.
Values may be sent and summed in bfloat16 or wider, within the bound.
A program may use at most 192 MiB of HBM per device.

```python
import math
import jax
import jax.numpy as jnp

D = 4608
FF = 18432
TOKENS = 256


def block_scale(rng, shape, cuts, low, top_value):
    def one(axis_at, blocks):
        draws = jax.random.uniform(jax.random.fold_in(jax.random.fold_in(rng, 6), axis_at), (blocks,), jnp.float32, low / len(cuts), top_value / len(cuts))
        return jnp.repeat(jnp.exp(draws), shape[axis_at] // blocks).reshape((-1,) + (1,) * (len(shape) - axis_at - 1))

    level = one(*cuts[0])
    for cut in cuts[1:]:
        level = level * one(*cut)
    return level


def centred(stream_key, shape, width, limit, shards=(), dtype=jnp.bfloat16):
    drawn = width * jax.random.normal(stream_key, shape, jnp.float32)
    if shards:
        drawn = drawn * block_scale(stream_key, shape, shards, -0.22, 0.18)
    return jnp.clip(drawn, -limit, limit).astype(dtype)


def setup_inputs(seed: int = 0) -> dict:
    key_list = jax.random.split(jax.random.key(seed), 6)
    normed = centred(key_list[0], (2, TOKENS, D), 1.0, 6.0, ((0, 2), (1, 4), (2, 4)))
    cotangent = centred(key_list[1], (2, TOKENS, D), 1.0, 6.0, ((0, 2), (1, 4), (2, 4)))
    w_gate = centred(key_list[2], (2, D, FF), D ** -0.5, 0.09375, ((0, 2), (1, 4), (2, 4)))
    w_up = centred(key_list[3], (2, D, FF), D ** -0.5, 0.09375, ((0, 2), (1, 4), (2, 4)))
    w_down = centred(key_list[4], (2, D, FF), FF ** -0.5, 0.046875, ((0, 2), (1, 4), (2, 4)))
    return {"normed": normed, "cotangent": cotangent, "w_gate": w_gate, "w_up": w_up, "w_down": w_down}


def activate(gate, up, back):
    coeff = math.sqrt(2.0 / math.pi)
    inner = jnp.tanh(coeff * (gate + 0.044715 * gate * gate * gate))
    act = 0.5 * gate * (1.0 + inner)
    slope = 0.5 * (1.0 + inner) + 0.5 * gate * (1.0 - inner * inner) * coeff * (1.0 + 3.0 * 0.044715 * gate * gate)
    hidden = (act * up).astype(jnp.bfloat16)
    d_gate = (back * up * slope).astype(jnp.bfloat16)
    d_up = (back * act).astype(jnp.bfloat16)
    return (hidden, d_gate, d_up)

def layer_back(rows, cot, wgate, wup, wdown):
    gate = jnp.dot(rows, wgate, preferred_element_type=jnp.float32)
    up = jnp.dot(rows, wup, preferred_element_type=jnp.float32)
    back = jnp.dot(cot, wdown, preferred_element_type=jnp.float32)
    hidden, d_gate, d_up = activate(gate, up, back)
    scale = 1.0 / math.sqrt(TOKENS)
    g_gate = (jnp.dot(rows.T, d_gate, preferred_element_type=jnp.float32) * scale).astype(jnp.bfloat16)
    g_up = (jnp.dot(rows.T, d_up, preferred_element_type=jnp.float32) * scale).astype(jnp.bfloat16)
    g_down = (jnp.dot(cot.T, hidden, preferred_element_type=jnp.float32) * scale).astype(jnp.bfloat16)
    branch = jnp.dot(d_gate, wgate.T, preferred_element_type=jnp.float32) + jnp.dot(d_up, wup.T, preferred_element_type=jnp.float32)
    handed = (cot.astype(jnp.float32) + branch).astype(jnp.bfloat16)
    return (handed, g_gate, g_up, g_down)

def reference(normed, cotangent, w_gate, w_up, w_down):
    first = layer_back(normed[0], cotangent[0], w_gate[0], w_up[0], w_down[0])
    second = layer_back(normed[1], cotangent[1], w_gate[1], w_up[1], w_down[1])
    passed = jnp.stack([second[0], first[0]])
    grad_gate = jnp.stack([first[1], second[1]])
    grad_up = jnp.stack([first[2], second[2]])
    grad_down = jnp.stack([first[3], second[3]])
    return (passed, grad_gate, grad_up, grad_down)
```

```python
import functools
import math

import jax
import jax.numpy as jnp
from jax import lax
from jax.experimental import pallas as pl
from jax.experimental.pallas import tpu as pltpu
from jax.sharding import PartitionSpec as P


MESH = pl.DeviceIdType.MESH
VMEM_LIMIT = 64 * 1024 * 1024 - 512 * 1024


def shift(value, axis, steps):
    count = lax.axis_size(axis)
    pairs = [(source, (source + steps) % count) for source in range(count)]
    return lax.ppermute(value, axis, pairs)


def wide(value):
    return value.astype(jnp.float32)


def gelu_parts(gate):
    coeff = math.sqrt(2.0 / math.pi)
    inner = jnp.tanh(coeff * (gate + 0.044715 * gate * gate * gate))
    act = 0.5 * gate * (1.0 + inner)
    slope = 0.5 * (1.0 + inner) + 0.5 * gate * (1.0 - inner * inner) * coeff * (
        1.0 + 3.0 * 0.044715 * gate * gate
    )
    return act, slope


def sum_kernel(
    tp, line, groups, window, lanes, sends, strip,
    n_own, c_own, w_gate, w_up, w_down,
    hidden_out, dgate_out, dup_out, nt_out, ct_out, branch_out,
    n_all, c_all, w_gu, w_dn, part, from_left, from_right, to_right, to_left, grads, acc, flip,
    n_send, n_recv, c_send, c_recv, w_sem, left_sem, right_sem, rsend_sem, lsend_sem, out_sem, flip_sem,
):
    rows = n_own.shape[0]
    total_rows = rows * tp
    width = n_own.shape[1]
    at = lax.axis_index("fsdp")
    mine = lax.axis_index("tp")
    first = at == 0
    last = at == line - 1
    left, right = at - 1, at + 1

    def columns(group):
        return pl.ds(pl.multiple_of(group * lanes, lanes), lanes)

    def weight_copies(group):
        slot = lax.rem(group, window)
        return (
            pltpu.make_async_copy(
                w_gate.at[0, :, columns(group)], w_gu.at[slot, :, pl.ds(0, lanes)], w_sem.at[slot, 0]
            ),
            pltpu.make_async_copy(
                w_up.at[0, :, columns(group)], w_gu.at[slot, :, pl.ds(lanes, lanes)], w_sem.at[slot, 1]
            ),
            pltpu.make_async_copy(w_down.at[0, :, columns(group)], w_dn.at[slot], w_sem.at[slot, 2]),
        )

    def right_copy(group, item):
        slot = lax.rem(group, sends)
        return pltpu.make_async_remote_copy(
            src_ref=to_right.at[slot, item], dst_ref=from_left.at[group, item],
            send_sem=rsend_sem.at[slot, item], recv_sem=left_sem.at[group, item],
            device_id={"fsdp": right}, device_id_type=MESH,
        )

    def left_copy(group, item):
        slot = lax.rem(group, sends)
        return pltpu.make_async_remote_copy(
            src_ref=to_left.at[slot, item], dst_ref=from_right.at[group, item],
            send_sem=lsend_sem.at[slot, item], recv_sem=right_sem.at[group, item],
            device_id={"fsdp": left}, device_id_type=MESH,
        )

    def out_copies(group):
        return [
            pltpu.make_async_copy(from_left.at[group, item], ref.at[:, columns(group)], out_sem.at[group, item])
            for item, ref in enumerate((hidden_out, dgate_out, dup_out))
        ]

    for group in range(window):
        for copy in weight_copies(group):
            copy.start()

    barrier = pltpu.get_barrier_semaphore()
    for step in range(1, tp):
        pl.semaphore_signal(barrier, inc=1, device_id={"tp": lax.rem(mine + step, tp)}, device_id_type=MESH)

    @pl.when(jnp.logical_not(first))
    def _():
        pl.semaphore_signal(barrier, inc=1, device_id={"fsdp": left}, device_id_type=MESH)

    @pl.when(jnp.logical_not(last))
    def _():
        pl.semaphore_signal(barrier, inc=1, device_id={"fsdp": right}, device_id_type=MESH)

    pl.semaphore_wait(barrier, tp - 1 + jnp.minimum(at, 1) + jnp.minimum(line - 1 - at, 1))

    def token_rows(index):
        return pl.ds(pl.multiple_of(index * rows, rows), rows)

    def gather_copies(own, everyone, send, recv):
        return [
            pltpu.make_async_remote_copy(
                src_ref=own, dst_ref=everyone.at[token_rows(mine)],
                send_sem=send.at[step - 1], recv_sem=recv.at[step - 1],
                device_id={"tp": lax.rem(mine + step, tp)}, device_id_type=MESH,
            )
            for step in range(1, tp)
        ]

    n_copies = gather_copies(n_own, n_all, n_send, n_recv)
    c_copies = gather_copies(c_own, c_all, c_send, c_recv)
    for copy in n_copies + c_copies:
        copy.start()
    n_all[token_rows(mine)] = n_own[...]
    c_all[token_rows(mine)] = c_own[...]
    acc[...] = jnp.zeros_like(acc)
    for copy in n_copies:
        copy.wait_recv()

    def send_on(copy, buffer, group, item, source, extra):
        slot = lax.rem(group, sends)

        @pl.when(group >= sends)
        def _():
            copy(group, item).wait_send()

        held = lax.rem(group, window)

        @pl.loop(0, total_rows, step=2 * strip)
        def _(start):
            span = pl.ds(pl.multiple_of(start, 2 * strip), 2 * strip)
            value = part[held, item, span]
            if source is not None:
                value = value + wide(source[group, item, span])
            buffer[slot, item, span] = value.astype(jnp.bfloat16)

        copy(group, item).start()

    lag = jnp.maximum(at, line - 1 - at)

    @pl.loop(0, groups + line - 1)
    def _(step):
        @pl.when(step < groups)
        def _():
            slot = lax.rem(step, window)
            gate_copy, up_copy, down_copy = weight_copies(step)
            gate_copy.wait()
            up_copy.wait()
            both = jnp.dot(n_all[...], w_gu[slot], preferred_element_type=jnp.float32)
            part[slot, 0] = both[:, :lanes]
            part[slot, 1] = both[:, lanes:]
            for item in range(3):
                if item == 2:
                    @pl.when(step == 0)
                    def _():
                        for copy in c_copies:
                            copy.wait_recv()

                    down_copy.wait()
                    part[slot, 2] = jnp.dot(c_all[...], w_dn[slot], preferred_element_type=jnp.float32)

                @pl.when(first)
                def _(item=item):
                    send_on(right_copy, to_right, step, item, None, None)

                @pl.when(last)
                def _(item=item):
                    send_on(left_copy, to_left, step, item, None, None)

        from_left_group = step - at
        from_right_group = step - (line - 1 - at)
        left_live = (at > 0) & (from_left_group >= 0) & (from_left_group < groups)
        right_live = (at < line - 1) & (from_right_group >= 0) & (from_right_group < groups)
        for item in range(3):
            @pl.when(left_live)
            def _(item=item):
                right_copy(from_left_group, item).wait_recv()

                @pl.when(jnp.logical_not(last))
                def _():
                    send_on(right_copy, to_right, from_left_group, item, from_left, None)

            @pl.when(right_live)
            def _(item=item):
                left_copy(from_right_group, item).wait_recv()

                @pl.when(jnp.logical_not(first))
                def _():
                    send_on(left_copy, to_left, from_right_group, item, from_right, None)

        done = step - lag

        @pl.when((done >= 0) & (done < groups))
        def _():
            slot = lax.rem(done, window)

            @pl.loop(0, total_rows, step=strip)
            def _(start):
                span = pl.ds(pl.multiple_of(start, strip), strip)

                def whole(item):
                    value = part[slot, item, span]
                    value = value + jnp.where(first, 0.0, wide(from_left[done, item, span]))
                    return value + jnp.where(last, 0.0, wide(from_right[done, item, span]))

                gate, up, back = whole(0), whole(1), whole(2)
                act, slope = gelu_parts(gate)
                d_gate = (back * up * slope).astype(jnp.bfloat16)
                d_up = (back * act).astype(jnp.bfloat16)
                from_left[done, 0, span] = (act * up).astype(jnp.bfloat16)
                from_left[done, 1, span] = d_gate
                from_left[done, 2, span] = d_up
                grads[span, pl.ds(0, lanes)] = d_gate
                grads[span, pl.ds(lanes, lanes)] = d_up

            for copy in out_copies(done):
                copy.start()
            acc[...] += lax.dot_general(
                grads[...], w_gu[slot], (((1,), (1,)), ((), ())), preferred_element_type=jnp.float32
            )

            @pl.when(done + window < groups)
            def _():
                for copy in weight_copies(done + window):
                    copy.start()

    flip[0] = n_all[...].T
    flip[1] = c_all[...].T
    flips = [
        pltpu.make_async_copy(flip.at[index], ref, flip_sem.at[index]) for index, ref in enumerate((nt_out, ct_out))
    ]
    for copy in flips:
        copy.start()
    branch_out[...] = acc[...].astype(jnp.bfloat16)

    for copy in n_copies + c_copies:
        copy.wait_send()

    @pl.loop(0, groups)
    def _(group):
        for copy in out_copies(group):
            copy.wait()

    @pl.loop(groups - sends, groups)
    def _(group):
        for item in range(3):
            @pl.when(jnp.logical_not(last))
            def _(item=item):
                right_copy(group, item).wait_send()

            @pl.when(jnp.logical_not(first))
            def _(item=item):
                left_copy(group, item).wait_send()

    for copy in flips:
        copy.wait()


def sum_and_activate(normed, cotangent, w_gate, w_up, w_down):
    tp, line = lax.axis_size("tp"), lax.axis_size("fsdp")
    rows, width = normed.shape
    hidden_units = w_gate.shape[2]
    tokens = rows * tp
    lanes = 256 if hidden_units % 256 == 0 and tokens <= 512 else 128
    groups = hidden_units // lanes
    window = min(groups, line + 2)
    sends = min(groups, 3)
    strip = 32
    dma = pltpu.SemaphoreType.DMA
    any_spec = pl.BlockSpec(memory_space=pl.ANY)
    vmem_spec = pl.BlockSpec(memory_space=pltpu.VMEM)
    wide_shape = jax.ShapeDtypeStruct((tokens, hidden_units), jnp.bfloat16)
    flip_shape = jax.ShapeDtypeStruct((width, tokens), jnp.bfloat16)
    half = jnp.bfloat16
    return pl.pallas_call(
        functools.partial(sum_kernel, tp, line, groups, window, lanes, sends, strip),
        out_shape=(
            wide_shape, wide_shape, wide_shape, flip_shape, flip_shape,
            jax.ShapeDtypeStruct((tokens, width), half),
        ),
        in_specs=[vmem_spec] * 2 + [any_spec] * 3,
        out_specs=(any_spec,) * 5 + (vmem_spec,),
        scratch_shapes=[
            pltpu.VMEM((tokens, width), half),
            pltpu.VMEM((tokens, width), half),
            pltpu.VMEM((window, width, 2 * lanes), half),
            pltpu.VMEM((window, width, lanes), half),
            pltpu.VMEM((window, 3, tokens, lanes), jnp.float32),
            pltpu.VMEM((groups, 3, tokens, lanes), half),
            pltpu.VMEM((groups, 3, tokens, lanes), half),
            pltpu.VMEM((sends, 3, tokens, lanes), half),
            pltpu.VMEM((sends, 3, tokens, lanes), half),
            pltpu.VMEM((tokens, 2 * lanes), half),
            pltpu.VMEM((tokens, width), jnp.float32),
            pltpu.VMEM((2, width, tokens), half),
            dma((tp - 1,)), dma((tp - 1,)), dma((tp - 1,)), dma((tp - 1,)),
            dma((window, 3)), dma((groups, 3)), dma((groups, 3)),
            dma((sends, 3)), dma((sends, 3)), dma((groups, 3)), dma((2,)),
        ],
        compiler_params=pltpu.CompilerParams(
            collective_id=0, has_side_effects=True, vmem_limit_bytes=VMEM_LIMIT
        ),
        name="line_sum",
    )(normed, cotangent, w_gate, w_up, w_down)


def grad_kernel(scale, left, *refs):
    half = len(refs) // 2
    for grad, out in zip(refs[:half], refs[half:]):
        value = jnp.dot(left[...], grad[...], preferred_element_type=jnp.float32)
        out[0] = (value * scale).astype(out.dtype)


def weight_grads(left, grads, scale):
    width, tokens = left.shape
    hidden_units = grads[0].shape[1]
    block = 512 if hidden_units % 512 == 0 else 256
    count = len(grads)
    return pl.pallas_call(
        functools.partial(grad_kernel, scale),
        grid=(hidden_units // block,),
        out_shape=[jax.ShapeDtypeStruct((1, width, hidden_units), jnp.bfloat16)] * count,
        in_specs=[pl.BlockSpec((width, tokens), lambda i: (0, 0))]
        + [pl.BlockSpec((tokens, block), lambda i: (0, i))] * count,
        out_specs=[pl.BlockSpec((1, width, block), lambda i: (0, 0, i))] * count,
        compiler_params=pltpu.CompilerParams(dimension_semantics=("arbitrary",)),
        cost_estimate=pl.CostEstimate(
            flops=2 * width * tokens * hidden_units * count,
            bytes_accessed=2 * hidden_units * (width + tokens) * count,
            transcendentals=0,
        ),
        name="weight_grads",
    )(left, *grads)


def local(normed, cotangent, w_gate, w_up, w_down):
    cot_own = cotangent[0]
    hidden, d_gate, d_up, rows_t, cot_t, branch = sum_and_activate(normed[0], cot_own, w_gate, w_up, w_down)
    scale = 1.0 / math.sqrt(rows_t.shape[1])
    own = cot_own.shape[0]
    tp = lax.axis_size("tp")
    me = lax.axis_index("tp")

    def block(step):
        return lax.dynamic_slice_in_dim(branch, lax.rem(me + step, tp) * own, own, 0)

    arrived = [shift(block(step), "tp", step) for step in range(1, tp)]
    grad_gate, grad_up = weight_grads(rows_t, (d_gate, d_up), scale)
    total = wide(cot_own) + wide(block(0))
    for item in arrived:
        total = total + wide(item)
    passed = shift(total.astype(jnp.bfloat16), "section", 1)
    (grad_down,) = weight_grads(cot_t, (hidden,), scale)
    return (passed[None], grad_gate, grad_up, grad_down)


def solution(mesh):
    in_specs = (
        P("section", "tp", "fsdp"),
        P("section", "tp", "fsdp"),
        P("section", "fsdp", "tp"),
        P("section", "fsdp", "tp"),
        P("section", "fsdp", "tp"),
    )
    out_specs = (
        P("section", "tp", "fsdp"),
        P("section", "fsdp", "tp"),
        P("section", "fsdp", "tp"),
        P("section", "fsdp", "tp"),
    )
    return jax.shard_map(local, mesh=mesh, in_specs=in_specs, out_specs=out_specs, check_vma=False)
```

```python
import functools
import math

import jax
import jax.numpy as jnp
from jax import lax
from jax.experimental import pallas as pl
from jax.experimental.pallas import tpu as pltpu
from jax.sharding import PartitionSpec as P


MESH = pl.DeviceIdType.MESH
VMEM_LIMIT = 64 * 1024 * 1024 - 512 * 1024


def shift(value, axis, steps):
    count = lax.axis_size(axis)
    pairs = [(source, (source + steps) % count) for source in range(count)]
    return lax.ppermute(value, axis, pairs)


def wide(value):
    return value.astype(jnp.float32)


def gelu_parts(gate):
    coeff = math.sqrt(2.0 / math.pi)
    inner = jnp.tanh(coeff * (gate + 0.044715 * gate * gate * gate))
    act = 0.5 * gate * (1.0 + inner)
    slope = 0.5 * (1.0 + inner) + 0.5 * gate * (1.0 - inner * inner) * coeff * (
        1.0 + 3.0 * 0.044715 * gate * gate
    )
    return act, slope


def sum_kernel(
    tp, line, groups, lanes, early, strip, scale,
    n_own, c_own, w_gate, w_up, w_down,
    hidden_out, dgate_out, dup_out, nt_out, ct_out, total_out,
    n_all, c_all, w_gu, w_dn, part, from_left, from_right, to_right, to_left, grads, acc, flip, sum_out, sum_in,
    n_send, n_recv, c_send, c_recv, gu_sem, dn_sem, left_sem, right_sem, rsend_sem, lsend_sem, out_sem, flip_sem,
    sum_send, sum_recv,
):
    rows = n_own.shape[0]
    steps = tp * groups
    window = w_gu.shape[0]
    down_window = w_dn.shape[0]
    sends = to_right.shape[0]
    outs = out_sem.shape[0]
    at = lax.axis_index("fsdp")
    mine = lax.axis_index("tp")
    first = at == 0
    last = at == line - 1
    left, right = at - 1, at + 1

    def place(step):
        later = step - early
        others = (step >= early) & (later < (tp - 1) * groups)
        turn = jnp.where(others, later // groups + 1, 0)
        group = jnp.where(others, lax.rem(later, groups), jnp.where(step < early, step, step - (tp - 1) * groups))
        return turn, group

    def columns(group):
        return pl.ds(pl.multiple_of(group * lanes, lanes), lanes)

    def token_rows(index):
        return pl.ds(pl.multiple_of(index * rows, rows), rows)

    def rows_of(turn):
        return token_rows(lax.rem(mine + turn, tp))

    def gu_copies(step):
        slot = lax.rem(step, window)
        span = columns(place(step)[1])
        return (
            pltpu.make_async_copy(w_gate.at[0, :, span], w_gu.at[slot, :, pl.ds(0, lanes)], gu_sem.at[slot, 0]),
            pltpu.make_async_copy(w_up.at[0, :, span], w_gu.at[slot, :, pl.ds(lanes, lanes)], gu_sem.at[slot, 1]),
        )

    def down_copy(step):
        slot = lax.rem(step, down_window)
        return pltpu.make_async_copy(w_down.at[0, :, columns(place(step)[1])], w_dn.at[slot], dn_sem.at[slot])

    def right_copy(step, item):
        slot = lax.rem(step, sends)
        return pltpu.make_async_remote_copy(
            src_ref=to_right.at[slot, item], dst_ref=from_left.at[step, item],
            send_sem=rsend_sem.at[slot, item], recv_sem=left_sem.at[step, item],
            device_id={"fsdp": right}, device_id_type=MESH,
        )

    def left_copy(step, item):
        slot = lax.rem(step, sends)
        return pltpu.make_async_remote_copy(
            src_ref=to_left.at[slot, item], dst_ref=from_right.at[step, item],
            send_sem=lsend_sem.at[slot, item], recv_sem=right_sem.at[step, item],
            device_id={"fsdp": left}, device_id_type=MESH,
        )

    def out_copies(step):
        turn, group = place(step)
        slot = lax.rem(step, outs)
        return [
            pltpu.make_async_copy(
                from_left.at[step, item], ref.at[rows_of(turn), columns(group)], out_sem.at[slot, item]
            )
            for item, ref in enumerate((hidden_out, dgate_out, dup_out))
        ]

    def sum_copy(turn):
        return pltpu.make_async_remote_copy(
            src_ref=sum_out.at[turn - 1], dst_ref=sum_in.at[turn - 1],
            send_sem=sum_send.at[turn - 1], recv_sem=sum_recv.at[turn - 1],
            device_id={"tp": lax.rem(mine + turn, tp)}, device_id_type=MESH,
        )

    for step in range(window):
        for copy in gu_copies(step):
            copy.start()
        if step < down_window:
            down_copy(step).start()

    barrier = pltpu.get_barrier_semaphore()
    for step in range(1, tp):
        pl.semaphore_signal(barrier, inc=1, device_id={"tp": lax.rem(mine + step, tp)}, device_id_type=MESH)

    @pl.when(jnp.logical_not(first))
    def _():
        pl.semaphore_signal(barrier, inc=1, device_id={"fsdp": left}, device_id_type=MESH)

    @pl.when(jnp.logical_not(last))
    def _():
        pl.semaphore_signal(barrier, inc=1, device_id={"fsdp": right}, device_id_type=MESH)

    n_all[token_rows(mine)] = n_own[...]
    c_all[token_rows(mine)] = c_own[...]
    acc[...] = jnp.zeros_like(acc)
    pl.semaphore_wait(barrier, tp - 1 + jnp.minimum(at, 1) + jnp.minimum(line - 1 - at, 1))

    def gather_copy(own, everyone, send, recv, turn):
        return pltpu.make_async_remote_copy(
            src_ref=own, dst_ref=everyone.at[token_rows(mine)],
            send_sem=send.at[turn - 1], recv_sem=recv.at[turn - 1],
            device_id={"tp": lax.rem(mine + tp - turn, tp)}, device_id_type=MESH,
        )

    def gathers(turn):
        return (
            gather_copy(n_own, n_all, n_send, n_recv, turn),
            gather_copy(c_own, c_all, c_send, c_recv, turn),
        )

    for turn in range(1, tp):
        for copy in gathers(turn):
            copy.start()

    def send_on(copy, buffer, step, item, source):
        slot = lax.rem(step, sends)
        held = lax.rem(step, window)

        @pl.when(step >= sends)
        def _():
            copy(step, item).wait_send()

        value = part[held, item]
        if source is not None:
            value = value + wide(source[step, item])
        buffer[slot, item] = value.astype(jnp.bfloat16)
        copy(step, item).start()

    def send_first(step, item):
        @pl.when(first)
        def _():
            send_on(right_copy, to_right, step, item, None)

        @pl.when(last)
        def _():
            send_on(left_copy, to_left, step, item, None)

    lag = jnp.maximum(at, line - 1 - at)

    @pl.loop(0, steps + line - 1)
    def _(step):
        @pl.when(step < steps)
        def _():
            turn, group = place(step)
            slot = lax.rem(step, window)

            @pl.when((turn > 0) & (group == 0))
            def _():
                for copy in gathers(turn):
                    copy.wait_recv()

            for copy in gu_copies(step):
                copy.wait()
            both = jnp.dot(n_all[rows_of(turn)], w_gu[slot], preferred_element_type=jnp.float32)
            part[slot, 0] = both[:, :lanes]
            part[slot, 1] = both[:, lanes:]
            send_first(step, 0)
            send_first(step, 1)
            down_copy(step).wait()
            part[slot, 2] = jnp.dot(
                c_all[rows_of(turn)], w_dn[lax.rem(step, down_window)], preferred_element_type=jnp.float32
            )
            send_first(step, 2)

            @pl.when(step + down_window < steps)
            def _():
                down_copy(step + down_window).start()

        left_step = step - at
        right_step = step - (line - 1 - at)
        left_live = (at > 0) & (left_step >= 0) & (left_step < steps)
        right_live = (at < line - 1) & (right_step >= 0) & (right_step < steps)
        for item in range(3):
            @pl.when(left_live)
            def _(item=item):
                right_copy(left_step, item).wait_recv()

                @pl.when(jnp.logical_not(last))
                def _():
                    send_on(right_copy, to_right, left_step, item, from_left)

            @pl.when(right_live)
            def _(item=item):
                left_copy(right_step, item).wait_recv()

                @pl.when(jnp.logical_not(first))
                def _():
                    send_on(left_copy, to_left, right_step, item, from_right)

        done = step - lag

        @pl.when((done >= 0) & (done < steps))
        def _():
            slot = lax.rem(done, window)
            turn, group = place(done)

            @pl.when(done >= outs)
            def _():
                for copy in out_copies(done - outs):
                    copy.wait()

            @pl.loop(0, rows, step=strip)
            def _(start):
                span = pl.ds(pl.multiple_of(start, strip), strip)

                def whole(item):
                    value = part[slot, item, span]
                    value = value + jnp.where(first, 0.0, wide(from_left[done, item, span]))
                    return value + jnp.where(last, 0.0, wide(from_right[done, item, span]))

                gate, up, back = whole(0), whole(1), whole(2)
                act, slope = gelu_parts(gate)
                d_gate = (back * up * slope).astype(jnp.bfloat16)
                d_up = (back * act).astype(jnp.bfloat16)
                from_left[done, 0, span] = (act * up).astype(jnp.bfloat16)
                from_left[done, 1, span] = d_gate
                from_left[done, 2, span] = d_up
                grads[span, pl.ds(0, lanes)] = d_gate
                grads[span, pl.ds(lanes, lanes)] = d_up

            for copy in out_copies(done):
                copy.start()
            kind = jnp.minimum(turn, 1)
            acc[kind] += lax.dot_general(
                grads[...], w_gu[slot], (((1,), (1,)), ((), ())), preferred_element_type=jnp.float32
            )

            @pl.when(done + window < steps)
            def _():
                for copy in gu_copies(done + window):
                    copy.start()

            @pl.when((turn > 0) & (group == groups - 1))
            def _():
                sum_out[turn - 1] = acc[1].astype(jnp.bfloat16)
                acc[1] = jnp.zeros_like(acc[1])
                sum_copy(turn).start()

            @pl.when((turn == tp - 1) & (group == 0))
            def _():
                flip[0] = (n_all[...] * scale).T
                flip[1] = (c_all[...] * scale).T
                for index, ref in enumerate((nt_out, ct_out)):
                    pltpu.make_async_copy(flip.at[index], ref, flip_sem.at[index]).start()

    total = wide(c_own[...]) + acc[0]
    for turn in range(1, tp):
        sum_copy(turn).wait_recv()
        total = total + wide(sum_in[turn - 1])
    total_out[...] = total.astype(jnp.bfloat16)

    for turn in range(1, tp):
        sum_copy(turn).wait_send()
        for copy in gathers(turn):
            copy.wait_send()

    @pl.loop(steps - outs, steps)
    def _(step):
        for copy in out_copies(step):
            copy.wait()

    @pl.loop(steps - sends, steps)
    def _(step):
        for item in range(3):
            @pl.when(jnp.logical_not(last))
            def _(item=item):
                right_copy(step, item).wait_send()

            @pl.when(jnp.logical_not(first))
            def _(item=item):
                left_copy(step, item).wait_send()

    for index, ref in enumerate((nt_out, ct_out)):
        pltpu.make_async_copy(flip.at[index], ref, flip_sem.at[index]).wait()


def sum_and_activate(normed, cotangent, w_gate, w_up, w_down, scale):
    tp, line = lax.axis_size("tp"), lax.axis_size("fsdp")
    rows, width = normed.shape
    hidden_units = w_gate.shape[2]
    tokens = rows * tp
    lanes = 512 if hidden_units % 512 == 0 else 256
    groups = hidden_units // lanes
    early = min(3, groups)
    steps = groups * tp
    window = line + 2
    sends = 3
    outs = 4
    dma = pltpu.SemaphoreType.DMA
    any_spec = pl.BlockSpec(memory_space=pl.ANY)
    vmem_spec = pl.BlockSpec(memory_space=pltpu.VMEM)
    half = jnp.bfloat16
    wide_shape = jax.ShapeDtypeStruct((tokens, hidden_units), half)
    flip_shape = jax.ShapeDtypeStruct((width, tokens), half)
    return pl.pallas_call(
        functools.partial(sum_kernel, tp, line, groups, lanes, early, 32, scale),
        out_shape=(
            wide_shape, wide_shape, wide_shape, flip_shape, flip_shape,
            jax.ShapeDtypeStruct((rows, width), half),
        ),
        in_specs=[vmem_spec] * 2 + [any_spec] * 3,
        out_specs=(any_spec,) * 5 + (vmem_spec,),
        scratch_shapes=[
            pltpu.VMEM((tokens, width), half),
            pltpu.VMEM((tokens, width), half),
            pltpu.VMEM((window, width, 2 * lanes), half),
            pltpu.VMEM((3, width, lanes), half),
            pltpu.VMEM((window, 3, rows, lanes), jnp.float32),
            pltpu.VMEM((steps, 3, rows, lanes), half),
            pltpu.VMEM((steps, 3, rows, lanes), half),
            pltpu.VMEM((sends, 3, rows, lanes), half),
            pltpu.VMEM((sends, 3, rows, lanes), half),
            pltpu.VMEM((rows, 2 * lanes), half),
            pltpu.VMEM((2, rows, width), jnp.float32),
            pltpu.VMEM((2, width, tokens), half),
            pltpu.VMEM((tp - 1, rows, width), half),
            pltpu.VMEM((tp - 1, rows, width), half),
            dma((tp - 1,)), dma((tp - 1,)), dma((tp - 1,)), dma((tp - 1,)),
            dma((window, 2)), dma((3,)), dma((steps, 3)), dma((steps, 3)),
            dma((sends, 3)), dma((sends, 3)), dma((outs, 3)), dma((2,)),
            dma((tp - 1,)), dma((tp - 1,)),
        ],
        compiler_params=pltpu.CompilerParams(
            collective_id=0, has_side_effects=True, vmem_limit_bytes=VMEM_LIMIT
        ),
        name="line_sum",
    )(normed, cotangent, w_gate, w_up, w_down)


def grad_kernel(scale, *refs):
    lefts, grads, outs = refs[:2], refs[2:5], refs[5:]
    for left, grad, out in zip((lefts[0], lefts[0], lefts[1]), grads, outs):
        value = jnp.dot(left[...], grad[...], preferred_element_type=jnp.float32)
        out[0] = (value if scale == 1.0 else value * scale).astype(out.dtype)


def weight_grads(rows_t, cot_t, d_gate, d_up, hidden, scale):
    width, tokens = rows_t.shape
    hidden_units = d_gate.shape[1]
    block = next(size for size in (1536, 768, 256, 128) if hidden_units % size == 0)
    return pl.pallas_call(
        functools.partial(grad_kernel, scale),
        grid=(hidden_units // block,),
        out_shape=[jax.ShapeDtypeStruct((1, width, hidden_units), jnp.bfloat16)] * 3,
        in_specs=[pl.BlockSpec((width, tokens), lambda i: (0, 0))] * 2
        + [pl.BlockSpec((tokens, block), lambda i: (0, i))] * 3,
        out_specs=[pl.BlockSpec((1, width, block), lambda i: (0, 0, i))] * 3,
        compiler_params=pltpu.CompilerParams(
            dimension_semantics=("arbitrary",), vmem_limit_bytes=60 * 1024 * 1024
        ),
        cost_estimate=pl.CostEstimate(
            flops=6 * width * tokens * hidden_units,
            bytes_accessed=6 * hidden_units * (width + tokens),
            transcendentals=0,
        ),
        name="weight_grads",
    )(rows_t, cot_t, d_gate, d_up, hidden)


def local(normed, cotangent, w_gate, w_up, w_down):
    scale = 1.0 / math.sqrt(normed.shape[1] * lax.axis_size("tp"))
    exact = math.frexp(scale)[0] == 0.5
    hidden, d_gate, d_up, rows_t, cot_t, total = sum_and_activate(
        normed[0], cotangent[0], w_gate, w_up, w_down, scale if exact else 1.0
    )
    passed = shift(total, "section", 1)
    grads = weight_grads(rows_t, cot_t, d_gate, d_up, hidden, 1.0 if exact else scale)
    return (passed[None], *grads)


def solution(mesh):
    in_specs = (
        P("section", "tp", "fsdp"),
        P("section", "tp", "fsdp"),
        P("section", "fsdp", "tp"),
        P("section", "fsdp", "tp"),
        P("section", "fsdp", "tp"),
    )
    out_specs = (
        P("section", "tp", "fsdp"),
        P("section", "fsdp", "tp"),
        P("section", "fsdp", "tp"),
        P("section", "fsdp", "tp"),
    )
    return jax.shard_map(local, mesh=mesh, in_specs=in_specs, out_specs=out_specs, check_vma=False)
```

```python
import functools
import math

import jax
import jax.numpy as jnp
from jax import lax
from jax.experimental import pallas as pl
from jax.experimental.pallas import tpu as pltpu
from jax.sharding import PartitionSpec as P


MESH = pl.DeviceIdType.MESH
VMEM_LIMIT = 52 * 1024 * 1024
HANDED_ELEMENTS = 4 * 1024 * 1024


def shift(value, axis, steps):
    count = lax.axis_size(axis)
    pairs = [(source, (source + steps) % count) for source in range(count)]
    return lax.ppermute(value, axis, pairs)


def wide(value):
    return value.astype(jnp.float32)


def gelu_parts(gate):
    coeff = math.sqrt(2.0 / math.pi)
    inner = jnp.tanh(coeff * (gate + 0.044715 * gate * gate * gate))
    act = 0.5 * gate * (1.0 + inner)
    slope = 0.5 * (1.0 + inner) + 0.5 * gate * (1.0 - inner * inner) * coeff * (
        1.0 + 3.0 * 0.044715 * gate * gate
    )
    return act, slope


def sum_kernel(
    tp, line, groups, lanes, early, strip, halves, direct, scale,
    n_own, c_own, w_gate, w_up, w_down,
    hidden_out, dgate_out, dup_out, nt_out, ct_out, total_out,
    n_all, c_all, w_gu, w_dn, part, from_left, from_right, to_right, to_left, grads, acc, sum_out, sum_in,
    n_send, n_recv, c_send, c_recv, gu_sem, dn_sem, left_sem, right_sem, rsend_sem, lsend_sem, out_sem, flip_sem,
    sum_send, sum_recv,
):
    rows = n_own.shape[0]
    steps = tp * groups
    piece = rows // halves
    window = w_gu.shape[0]
    down_window = w_dn.shape[0]
    sends = to_right.shape[0]
    outs = out_sem.shape[0]
    at = lax.axis_index("fsdp")
    mine = lax.axis_index("tp")
    first = at == 0
    last = at == line - 1
    left, right = at - 1, at + 1

    def place(step):
        later = step - early
        others = (step >= early) & (later < (tp - 1) * groups)
        turn = jnp.where(others, later // groups + 1, 0)
        group = jnp.where(others, lax.rem(later, groups), jnp.where(step < early, step, step - (tp - 1) * groups))
        return turn, group

    def columns(group):
        return pl.ds(pl.multiple_of(group * lanes, lanes), lanes)

    def token_rows(index):
        return pl.ds(pl.multiple_of(index * rows, rows), rows)

    def half_rows(half):
        return pl.ds(half * piece, piece)

    def rows_of(turn):
        return token_rows(lax.rem(mine + turn, tp))

    def gu_copies(step):
        slot = lax.rem(step, window)
        span = columns(place(step)[1])
        return (
            pltpu.make_async_copy(w_gate.at[0, :, span], w_gu.at[slot, :, pl.ds(0, lanes)], gu_sem.at[slot, 0]),
            pltpu.make_async_copy(w_up.at[0, :, span], w_gu.at[slot, :, pl.ds(lanes, lanes)], gu_sem.at[slot, 1]),
        )

    def down_copy(step):
        slot = lax.rem(step, down_window)
        return pltpu.make_async_copy(w_down.at[0, :, columns(place(step)[1])], w_dn.at[slot], dn_sem.at[slot])

    def right_copy(step, item, half):
        slot = lax.rem(step, sends)
        return pltpu.make_async_remote_copy(
            src_ref=to_right.at[slot, item, half_rows(half)], dst_ref=from_left.at[step, item, half_rows(half)],
            send_sem=rsend_sem.at[slot, item, half], recv_sem=left_sem.at[step, item, half],
            device_id={"fsdp": right}, device_id_type=MESH,
        )

    def left_copy(step, item, half):
        slot = lax.rem(step, sends)
        return pltpu.make_async_remote_copy(
            src_ref=to_left.at[slot, item, half_rows(half)], dst_ref=from_right.at[step, item, half_rows(half)],
            send_sem=lsend_sem.at[slot, item, half], recv_sem=right_sem.at[step, item, half],
            device_id={"fsdp": left}, device_id_type=MESH,
        )

    def out_copies(step):
        turn, group = place(step)
        slot = lax.rem(step, outs)
        return [
            pltpu.make_async_copy(
                from_left.at[step, item], ref.at[rows_of(turn), columns(group)], out_sem.at[slot, item]
            )
            for item, ref in enumerate((hidden_out, dgate_out, dup_out))
        ]

    def sum_copy(turn):
        return pltpu.make_async_remote_copy(
            src_ref=sum_out.at[turn - 1], dst_ref=sum_in.at[turn - 1],
            send_sem=sum_send.at[turn - 1], recv_sem=sum_recv.at[turn - 1],
            device_id={"tp": lax.rem(mine + turn, tp)}, device_id_type=MESH,
        )

    own_copies = [
        pltpu.make_async_copy(own, everyone.at[token_rows(mine)], flip_sem.at[index])
        for index, (own, everyone) in enumerate(((n_own, n_all), (c_own, c_all)))
    ]
    for copy in own_copies:
        copy.start()
    ahead = min(2, window)
    for step in range(ahead):
        for copy in gu_copies(step):
            copy.start()
        down_copy(step).start()

    barrier = pltpu.get_barrier_semaphore()
    for step in range(1, tp):
        pl.semaphore_signal(barrier, inc=1, device_id={"tp": lax.rem(mine + step, tp)}, device_id_type=MESH)

    @pl.when(jnp.logical_not(first))
    def _():
        pl.semaphore_signal(barrier, inc=1, device_id={"fsdp": left}, device_id_type=MESH)

    @pl.when(jnp.logical_not(last))
    def _():
        pl.semaphore_signal(barrier, inc=1, device_id={"fsdp": right}, device_id_type=MESH)

    acc[...] = jnp.zeros_like(acc)
    for copy in own_copies:
        copy.wait()
    pl.semaphore_wait(barrier, tp - 1 + jnp.minimum(at, 1) + jnp.minimum(line - 1 - at, 1))

    def gather_copy(everyone, send, recv, turn):
        return pltpu.make_async_remote_copy(
            src_ref=everyone.at[token_rows(mine)], dst_ref=everyone.at[token_rows(mine)],
            send_sem=send.at[turn - 1], recv_sem=recv.at[turn - 1],
            device_id={"tp": lax.rem(mine + tp - turn, tp)}, device_id_type=MESH,
        )

    def gathers(turn):
        return (
            gather_copy(n_all, n_send, n_recv, turn),
            gather_copy(c_all, c_send, c_recv, turn),
        )

    for turn in range(1, tp):
        for copy in gathers(turn):
            copy.start()

    def send_on(copy, buffer, step, item, half, source):
        slot = lax.rem(step, sends)
        held = lax.rem(step, window)

        @pl.when(step >= sends)
        def _():
            copy(step, item, half).wait_send()

        value = part[held, item, half_rows(half)]
        if source is not None:
            value = value + wide(source[step, item, half_rows(half)])
        buffer[slot, item, half_rows(half)] = value.astype(jnp.bfloat16)
        copy(step, item, half).start()

    def send_first(step, item):
        for half in range(halves):
            @pl.when(first)
            def _(half=half):
                send_on(right_copy, to_right, step, item, half, None)

            @pl.when(last)
            def _(half=half):
                send_on(left_copy, to_left, step, item, half, None)

    lag = jnp.maximum(at, line - 1 - at)

    @pl.loop(0, steps + line - 1)
    def _(step):
        left_step = step - at
        right_step = step - (line - 1 - at)
        left_live = (at > 0) & (left_step >= 0) & (left_step < steps)
        right_live = (at < line - 1) & (right_step >= 0) & (right_step < steps)

        def pass_half(item, half):
            @pl.when(left_live)
            def _():
                right_copy(left_step, item, half).wait_recv()

                @pl.when(jnp.logical_not(last))
                def _():
                    send_on(right_copy, to_right, left_step, item, half, from_left)

            @pl.when(right_live)
            def _():
                left_copy(right_step, item, half).wait_recv()

                @pl.when(jnp.logical_not(first))
                def _():
                    send_on(left_copy, to_left, right_step, item, half, from_right)

        def pass_on(item):
            for half in range(halves):
                pass_half(item, half)

        pass_on(0)

        @pl.when(step < steps)
        def _():
            turn, group = place(step)
            slot = lax.rem(step, window)

            @pl.when((turn > 0) & (group == 0))
            def _():
                for copy in gathers(turn):
                    copy.wait_recv()

            for copy in gu_copies(step):
                copy.wait()
            both = jnp.dot(n_all[rows_of(turn)], w_gu[slot], preferred_element_type=jnp.float32)
            part[slot, 0] = both[:, :lanes]
            part[slot, 1] = both[:, lanes:]
            send_first(step, 0)
            send_first(step, 1)

            @pl.when(step == 0)
            def _():
                for later in range(ahead, window):
                    for copy in gu_copies(later):
                        copy.start()
                for later in range(ahead, down_window):
                    down_copy(later).start()

        pass_on(1)

        @pl.when(step < steps)
        def _():
            turn = place(step)[0]
            down_copy(step).wait()
            part[lax.rem(step, window), 2] = jnp.dot(
                c_all[rows_of(turn)], w_dn[lax.rem(step, down_window)], preferred_element_type=jnp.float32
            )
            send_first(step, 2)

            @pl.when(step + down_window < steps)
            def _():
                down_copy(step + down_window).start()

        pass_on(2)

        done = step - lag

        @pl.when((done >= 0) & (done < steps))
        def _():
            slot = lax.rem(done, window)
            turn, group = place(done)

            base = lax.rem(mine + turn, tp) * rows
            if not direct:
                @pl.when(done >= outs)
                def _():
                    for copy in out_copies(done - outs):
                        copy.wait()

            @pl.loop(0, rows, step=strip)
            def _(start):
                span = pl.ds(pl.multiple_of(start, strip), strip)

                def whole(item):
                    value = part[slot, item, span]
                    value = value + jnp.where(first, 0.0, wide(from_left[done, item, span]))
                    return value + jnp.where(last, 0.0, wide(from_right[done, item, span]))

                gate, up, back = whole(0), whole(1), whole(2)
                act, slope = gelu_parts(gate)
                d_gate = (back * up * slope).astype(jnp.bfloat16)
                d_up = (back * act).astype(jnp.bfloat16)
                results = ((act * up).astype(jnp.bfloat16), d_gate, d_up)
                for item, (ref, result) in enumerate(zip((hidden_out, dgate_out, dup_out), results)):
                    if direct:
                        ref[pl.ds(pl.multiple_of(base + start, strip), strip), columns(group)] = result
                    else:
                        from_left[done, item, span] = result
                grads[span, pl.ds(0, lanes)] = d_gate
                grads[span, pl.ds(lanes, lanes)] = d_up

            if not direct:
                for copy in out_copies(done):
                    copy.start()
            kind = jnp.minimum(turn, 1)
            acc[kind] += lax.dot_general(
                grads[...], w_gu[slot], (((1,), (1,)), ((), ())), preferred_element_type=jnp.float32
            )

            @pl.when(done + window < steps)
            def _():
                for copy in gu_copies(done + window):
                    copy.start()

            @pl.when((turn > 0) & (group == groups - 1))
            def _():
                sum_out[turn - 1] = acc[1].astype(jnp.bfloat16)
                acc[1] = jnp.zeros_like(acc[1])
                sum_copy(turn).start()

            @pl.when((turn == tp - 1) & (group == 0))
            def _():
                nt_out[...] = (n_all[...] * scale).T
                ct_out[...] = (c_all[...] * scale).T

    total = wide(c_all[token_rows(mine)]) + acc[0]
    for turn in range(1, tp):
        sum_copy(turn).wait_recv()
        total = total + wide(sum_in[turn - 1])
    total_out[...] = total.astype(jnp.bfloat16)

    for turn in range(1, tp):
        sum_copy(turn).wait_send()
        for copy in gathers(turn):
            copy.wait_send()

    if not direct:
        @pl.loop(steps - outs, steps)
        def _(step):
            for copy in out_copies(step):
                copy.wait()

    @pl.loop(steps - sends, steps)
    def _(step):
        for item in range(3):
            for half in range(halves):
                @pl.when(jnp.logical_not(last))
                def _(item=item, half=half):
                    right_copy(step, item, half).wait_send()

                @pl.when(jnp.logical_not(first))
                def _(item=item, half=half):
                    left_copy(step, item, half).wait_send()


def sum_and_activate(normed, cotangent, w_gate, w_up, w_down, scale):
    tp, line = lax.axis_size("tp"), lax.axis_size("fsdp")
    rows, width = normed.shape
    hidden_units = w_gate.shape[2]
    tokens = rows * tp
    lanes = 512 if hidden_units % 512 == 0 else 256
    groups = hidden_units // lanes
    early = min(3, groups)
    steps = groups * tp
    window = line + 2
    sends = 3
    outs = 4
    dma = pltpu.SemaphoreType.DMA
    any_spec = pl.BlockSpec(memory_space=pl.ANY)
    vmem_spec = pl.BlockSpec(memory_space=pltpu.VMEM)
    half = jnp.bfloat16
    direct = 3 * tokens * hidden_units <= HANDED_ELEMENTS
    halves = 2 if direct else 1
    wide_shape = (pltpu.VMEM if direct else jax.ShapeDtypeStruct)((tokens, hidden_units), half)
    flip_shape = pltpu.VMEM((width, tokens), half)
    return pl.pallas_call(
        functools.partial(sum_kernel, tp, line, groups, lanes, early, 16, halves, direct, scale),
        out_shape=(
            wide_shape, wide_shape, wide_shape, flip_shape, flip_shape,
            pltpu.VMEM((rows, width), half),
        ),
        in_specs=[any_spec] * 5,
        out_specs=(vmem_spec if direct else any_spec,) * 3 + (vmem_spec,) * 3,
        scratch_shapes=[
            pltpu.VMEM((tokens, width), half),
            pltpu.VMEM((tokens, width), half),
            pltpu.VMEM((window, width, 2 * lanes), half),
            pltpu.VMEM((3, width, lanes), half),
            pltpu.VMEM((window, 3, rows, lanes), jnp.float32),
            pltpu.VMEM((steps, 3, rows, lanes), half),
            pltpu.VMEM((steps, 3, rows, lanes), half),
            pltpu.VMEM((sends, 3, rows, lanes), half),
            pltpu.VMEM((sends, 3, rows, lanes), half),
            pltpu.VMEM((rows, 2 * lanes), half),
            pltpu.VMEM((2, rows, width), jnp.float32),
            pltpu.VMEM((tp - 1, rows, width), half),
            pltpu.VMEM((tp - 1, rows, width), half),
            dma((tp - 1,)), dma((tp - 1,)), dma((tp - 1,)), dma((tp - 1,)),
            dma((window, 2)), dma((3,)), dma((steps, 3, halves)), dma((steps, 3, halves)),
            dma((sends, 3, halves)), dma((sends, 3, halves)), dma((outs, 3)), dma((2,)),
            dma((tp - 1,)), dma((tp - 1,)),
        ],
        compiler_params=pltpu.CompilerParams(
            collective_id=0, has_side_effects=True, vmem_limit_bytes=VMEM_LIMIT
        ),
        name="line_sum",
    )(normed, cotangent, w_gate, w_up, w_down)


def grad_kernel(scale, *refs):
    lefts, grads, outs = refs[:2], refs[2:5], refs[5:]
    for left, grad, out in zip((lefts[0], lefts[0], lefts[1]), grads, outs):
        value = jnp.dot(left[...], grad[...], preferred_element_type=jnp.float32)
        out[0] = (value if scale == 1.0 else value * scale).astype(out.dtype)


def weight_grads(rows_t, cot_t, d_gate, d_up, hidden, scale):
    width, tokens = rows_t.shape
    hidden_units = d_gate.shape[1]
    block = next(size for size in (768, 256, 128) if hidden_units % size == 0)
    return pl.pallas_call(
        functools.partial(grad_kernel, scale),
        grid=(hidden_units // block,),
        out_shape=[jax.ShapeDtypeStruct((1, width, hidden_units), jnp.bfloat16)] * 3,
        in_specs=[pl.BlockSpec((width, tokens), lambda i: (0, 0))] * 2
        + [pl.BlockSpec((tokens, block), lambda i: (0, i))] * 3,
        out_specs=[pl.BlockSpec((1, width, block), lambda i: (0, 0, i))] * 3,
        compiler_params=pltpu.CompilerParams(
            dimension_semantics=("arbitrary",), vmem_limit_bytes=40 * 1024 * 1024
        ),
        cost_estimate=pl.CostEstimate(
            flops=6 * width * tokens * hidden_units,
            bytes_accessed=6 * hidden_units * (width + tokens),
            transcendentals=0,
        ),
        name="weight_grads",
    )(rows_t, cot_t, d_gate, d_up, hidden)


def local(normed, cotangent, w_gate, w_up, w_down):
    scale = 1.0 / math.sqrt(normed.shape[1] * lax.axis_size("tp"))
    exact = math.frexp(scale)[0] == 0.5
    hidden, d_gate, d_up, rows_t, cot_t, total = sum_and_activate(
        normed[0], cotangent[0], w_gate, w_up, w_down, scale if exact else 1.0
    )
    passed = shift(total, "section", 1)
    grads = weight_grads(rows_t, cot_t, d_gate, d_up, hidden, 1.0 if exact else scale)
    return (passed[None], *grads)


def solution(mesh):
    in_specs = (
        P("section", "tp", "fsdp"),
        P("section", "tp", "fsdp"),
        P("section", "fsdp", "tp"),
        P("section", "fsdp", "tp"),
        P("section", "fsdp", "tp"),
    )
    out_specs = (
        P("section", "tp", "fsdp"),
        P("section", "fsdp", "tp"),
        P("section", "fsdp", "tp"),
        P("section", "fsdp", "tp"),
    )
    return jax.shard_map(local, mesh=mesh, in_specs=in_specs, out_specs=out_specs, check_vma=False)
```

```python
import functools
import math

import jax
import jax.numpy as jnp
from jax import lax
from jax.experimental import pallas as pl
from jax.experimental.pallas import tpu as pltpu
from jax.sharding import PartitionSpec as P


MESH = pl.DeviceIdType.MESH
VMEM_LIMIT = 52 * 1024 * 1024
HANDED_ELEMENTS = 4 * 1024 * 1024


def shift(value, axis, steps):
    count = lax.axis_size(axis)
    pairs = [(source, (source + steps) % count) for source in range(count)]
    return lax.ppermute(value, axis, pairs)


def wide(value):
    return value.astype(jnp.float32)


def gelu_parts(gate):
    coeff = math.sqrt(2.0 / math.pi)
    inner = jnp.tanh(coeff * (gate + 0.044715 * gate * gate * gate))
    act = 0.5 * gate * (1.0 + inner)
    slope = 0.5 * (1.0 + inner) + 0.5 * gate * (1.0 - inner * inner) * coeff * (
        1.0 + 3.0 * 0.044715 * gate * gate
    )
    return act, slope


def sum_kernel(
    tp, line, groups, lanes, early, strip, halves, direct, scale,
    n_own, c_own, w_gate, w_up, w_down,
    hidden_out, dgate_out, dup_out, nt_out, ct_out, total_out,
    n_all, c_all, w_gu, w_dn, part, from_left, from_right, to_right, to_left, grads, acc, sum_out, sum_in,
    n_send, n_recv, c_send, c_recv, gu_sem, dn_sem, left_sem, right_sem, rsend_sem, lsend_sem, out_sem, flip_sem,
    sum_send, sum_recv,
):
    rows = n_own.shape[0]
    steps = tp * groups
    width = n_own.shape[1]
    piece = rows // halves
    window = w_gu.shape[0]
    down_window = w_dn.shape[0]
    sends = to_right.shape[0]
    outs = out_sem.shape[0]
    at = lax.axis_index("fsdp")
    mine = lax.axis_index("tp")
    first = at == 0
    last = at == line - 1
    left, right = at - 1, at + 1

    def place(step):
        later = step - early
        others = (step >= early) & (later < (tp - 1) * groups)
        turn = jnp.where(others, later // groups + 1, 0)
        group = jnp.where(others, lax.rem(later, groups), jnp.where(step < early, step, step - (tp - 1) * groups))
        return turn, group

    def columns(group):
        return pl.ds(pl.multiple_of(group * lanes, lanes), lanes)

    def token_rows(index):
        return pl.ds(pl.multiple_of(index * rows, rows), rows)

    def half_rows(half):
        return pl.ds(half * piece, piece)

    def rows_of(turn):
        return token_rows(lax.rem(mine + turn, tp))

    def gu_copies(step):
        slot = lax.rem(step, window)
        span = columns(place(step)[1])
        return (
            pltpu.make_async_copy(w_gate.at[0, :, span], w_gu.at[slot, :, pl.ds(0, lanes)], gu_sem.at[slot, 0]),
            pltpu.make_async_copy(w_up.at[0, :, span], w_gu.at[slot, :, pl.ds(lanes, lanes)], gu_sem.at[slot, 1]),
        )

    def down_copy(step):
        slot = lax.rem(step, down_window)
        return pltpu.make_async_copy(w_down.at[0, :, columns(place(step)[1])], w_dn.at[slot], dn_sem.at[slot])

    def right_copy(step, item, half):
        slot = lax.rem(step, sends)
        return pltpu.make_async_remote_copy(
            src_ref=to_right.at[slot, item, half_rows(half)], dst_ref=from_left.at[step, item, half_rows(half)],
            send_sem=rsend_sem.at[slot, item, half], recv_sem=left_sem.at[step, item, half],
            device_id={"fsdp": right}, device_id_type=MESH,
        )

    def left_copy(step, item, half):
        slot = lax.rem(step, sends)
        return pltpu.make_async_remote_copy(
            src_ref=to_left.at[slot, item, half_rows(half)], dst_ref=from_right.at[step, item, half_rows(half)],
            send_sem=lsend_sem.at[slot, item, half], recv_sem=right_sem.at[step, item, half],
            device_id={"fsdp": left}, device_id_type=MESH,
        )

    def out_copies(step):
        turn, group = place(step)
        slot = lax.rem(step, outs)
        return [
            pltpu.make_async_copy(
                from_left.at[step, item], ref.at[rows_of(turn), columns(group)], out_sem.at[slot, item]
            )
            for item, ref in enumerate((hidden_out, dgate_out, dup_out))
        ]

    def sum_copy(turn):
        return pltpu.make_async_remote_copy(
            src_ref=sum_out.at[turn - 1], dst_ref=sum_in.at[turn - 1],
            send_sem=sum_send.at[turn - 1], recv_sem=sum_recv.at[turn - 1],
            device_id={"tp": lax.rem(mine + turn, tp)}, device_id_type=MESH,
        )

    own_copies = [
        pltpu.make_async_copy(own, everyone.at[token_rows(mine)], flip_sem.at[index])
        for index, (own, everyone) in enumerate(((n_own, n_all), (c_own, c_all)))
    ]
    for copy in own_copies:
        copy.start()
    ahead = min(2, window)
    for step in range(ahead):
        for copy in gu_copies(step):
            copy.start()
        down_copy(step).start()

    barrier = pltpu.get_barrier_semaphore()
    for step in range(1, tp):
        pl.semaphore_signal(barrier, inc=1, device_id={"tp": lax.rem(mine + step, tp)}, device_id_type=MESH)

    @pl.when(jnp.logical_not(first))
    def _():
        pl.semaphore_signal(barrier, inc=1, device_id={"fsdp": left}, device_id_type=MESH)

    @pl.when(jnp.logical_not(last))
    def _():
        pl.semaphore_signal(barrier, inc=1, device_id={"fsdp": right}, device_id_type=MESH)

    acc[...] = jnp.zeros_like(acc)
    for copy in own_copies:
        copy.wait()
    pl.semaphore_wait(barrier, tp - 1 + jnp.minimum(at, 1) + jnp.minimum(line - 1 - at, 1))

    def gather_copy(everyone, send, recv, turn):
        return pltpu.make_async_remote_copy(
            src_ref=everyone.at[token_rows(mine)], dst_ref=everyone.at[token_rows(mine)],
            send_sem=send.at[turn - 1], recv_sem=recv.at[turn - 1],
            device_id={"tp": lax.rem(mine + tp - turn, tp)}, device_id_type=MESH,
        )

    def gathers(turn):
        return (
            gather_copy(n_all, n_send, n_recv, turn),
            gather_copy(c_all, c_send, c_recv, turn),
        )

    for turn in range(1, tp):
        for copy in gathers(turn):
            copy.start()

    def send_on(copy, buffer, step, item, half, source):
        slot = lax.rem(step, sends)
        held = lax.rem(step, window)

        @pl.when(step >= sends)
        def _():
            copy(step, item, half).wait_send()

        value = part[held, item, half_rows(half)]
        if source is not None:
            value = value + wide(source[step, item, half_rows(half)])
        buffer[slot, item, half_rows(half)] = value.astype(jnp.bfloat16)
        copy(step, item, half).start()

    def send_first(step, item):
        for half in range(halves):
            @pl.when(first)
            def _(half=half):
                send_on(right_copy, to_right, step, item, half, None)

            @pl.when(last)
            def _(half=half):
                send_on(left_copy, to_left, step, item, half, None)

    lag = jnp.maximum(at, line - 1 - at)

    @pl.loop(0, steps + line - 1)
    def _(step):
        left_step = step - at
        right_step = step - (line - 1 - at)
        left_live = (at > 0) & (left_step >= 0) & (left_step < steps)
        right_live = (at < line - 1) & (right_step >= 0) & (right_step < steps)

        def pass_right(item, half, live):
            @pl.when(live)
            def _():
                right_copy(left_step, item, half).wait_recv()

                @pl.when(jnp.logical_not(last))
                def _():
                    send_on(right_copy, to_right, left_step, item, half, from_left)

        def pass_half(item, half):
            pass_right(item, half, left_live & (at >= line - 1 - at))

            @pl.when(right_live)
            def _():
                left_copy(right_step, item, half).wait_recv()

                @pl.when(jnp.logical_not(first))
                def _():
                    send_on(left_copy, to_left, right_step, item, half, from_right)

            pass_right(item, half, left_live & (at < line - 1 - at))

        def pass_on(item):
            for half in range(halves):
                pass_half(item, half)

        pass_on(0)

        @pl.when(step < steps)
        def _():
            turn, group = place(step)
            slot = lax.rem(step, window)

            @pl.when((turn > 0) & (group == 0))
            def _():
                for copy in gathers(turn):
                    copy.wait_recv()

            for item, copy in enumerate(gu_copies(step)):
                copy.wait()
                part[slot, item] = jnp.dot(
                    n_all[rows_of(turn)],
                    w_gu[slot, :, item * lanes : (item + 1) * lanes],
                    preferred_element_type=jnp.float32,
                )
                send_first(step, item)

            @pl.when(step == 0)
            def _():
                for later in range(ahead, window):
                    for copy in gu_copies(later):
                        copy.start()
                for later in range(ahead, down_window):
                    down_copy(later).start()

        pass_on(1)

        @pl.when(step < steps)
        def _():
            turn = place(step)[0]
            down_copy(step).wait()
            part[lax.rem(step, window), 2] = jnp.dot(
                c_all[rows_of(turn)], w_dn[lax.rem(step, down_window)], preferred_element_type=jnp.float32
            )
            send_first(step, 2)

            @pl.when(step + down_window < steps)
            def _():
                down_copy(step + down_window).start()

        pass_on(2)

        done = step - lag

        @pl.when((done >= 0) & (done < steps))
        def _():
            slot = lax.rem(done, window)
            turn, group = place(done)

            base = lax.rem(mine + turn, tp) * rows
            if not direct:
                @pl.when(done >= outs)
                def _():
                    for copy in out_copies(done - outs):
                        copy.wait()

            @pl.loop(0, rows, step=strip)
            def _(start):
                span = pl.ds(pl.multiple_of(start, strip), strip)

                def whole(item):
                    value = part[slot, item, span]
                    value = value + jnp.where(first, 0.0, wide(from_left[done, item, span]))
                    return value + jnp.where(last, 0.0, wide(from_right[done, item, span]))

                gate, up, back = whole(0), whole(1), whole(2)
                act, slope = gelu_parts(gate)
                d_gate = (back * up * slope).astype(jnp.bfloat16)
                d_up = (back * act).astype(jnp.bfloat16)
                results = ((act * up).astype(jnp.bfloat16), d_gate, d_up)
                for item, (ref, result) in enumerate(zip((hidden_out, dgate_out, dup_out), results)):
                    if direct:
                        ref[pl.ds(pl.multiple_of(base + start, strip), strip), columns(group)] = result
                    else:
                        from_left[done, item, span] = result
                grads[span, pl.ds(0, lanes)] = d_gate
                grads[span, pl.ds(lanes, lanes)] = d_up

            if not direct:
                for copy in out_copies(done):
                    copy.start()
            kind = jnp.minimum(turn, 1)
            acc[kind] += lax.dot_general(
                grads[...], w_gu[slot], (((1,), (1,)), ((), ())), preferred_element_type=jnp.float32
            )

            @pl.when(done + window < steps)
            def _():
                for copy in gu_copies(done + window):
                    copy.start()

            @pl.when((turn > 0) & (group == groups - 1))
            def _():
                sum_out[turn - 1] = acc[1].astype(jnp.bfloat16)
                acc[1] = jnp.zeros_like(acc[1])
                sum_copy(turn).start()

            slab = width // groups if width % (groups * 128) == 0 else width

            @pl.when((turn == tp - 1) & (group < width // slab))
            def _():
                span = pl.ds(0 if slab == width else pl.multiple_of(group * slab, slab), slab)
                nt_out[span] = (n_all[:, span] * scale).T
                ct_out[span] = (c_all[:, span] * scale).T

    total = wide(c_all[token_rows(mine)]) + acc[0]
    for turn in range(1, tp):
        sum_copy(turn).wait_recv()
        total = total + wide(sum_in[turn - 1])
    total_out[...] = total.astype(jnp.bfloat16)

    for turn in range(1, tp):
        sum_copy(turn).wait_send()
        for copy in gathers(turn):
            copy.wait_send()

    if not direct:
        @pl.loop(steps - outs, steps)
        def _(step):
            for copy in out_copies(step):
                copy.wait()

    @pl.loop(steps - sends, steps)
    def _(step):
        for item in range(3):
            for half in range(halves):
                @pl.when(jnp.logical_not(last))
                def _(item=item, half=half):
                    right_copy(step, item, half).wait_send()

                @pl.when(jnp.logical_not(first))
                def _(item=item, half=half):
                    left_copy(step, item, half).wait_send()


def sum_and_activate(normed, cotangent, w_gate, w_up, w_down, scale):
    tp, line = lax.axis_size("tp"), lax.axis_size("fsdp")
    rows, width = normed.shape
    hidden_units = w_gate.shape[2]
    tokens = rows * tp
    lanes = 512 if hidden_units % 512 == 0 else 256
    groups = hidden_units // lanes
    early = min(4, groups)
    steps = groups * tp
    window = line + 2
    sends = 3
    outs = 4
    dma = pltpu.SemaphoreType.DMA
    any_spec = pl.BlockSpec(memory_space=pl.ANY)
    vmem_spec = pl.BlockSpec(memory_space=pltpu.VMEM)
    half = jnp.bfloat16
    direct = 3 * tokens * hidden_units <= HANDED_ELEMENTS
    halves = 1
    wide_shape = (pltpu.VMEM if direct else jax.ShapeDtypeStruct)((tokens, hidden_units), half)
    flip_shape = pltpu.VMEM((width, tokens), half)
    return pl.pallas_call(
        functools.partial(sum_kernel, tp, line, groups, lanes, early, 16, halves, direct, scale),
        out_shape=(
            wide_shape, wide_shape, wide_shape, flip_shape, flip_shape,
            pltpu.VMEM((rows, width), half),
        ),
        in_specs=[any_spec] * 5,
        out_specs=(vmem_spec if direct else any_spec,) * 3 + (vmem_spec,) * 3,
        scratch_shapes=[
            pltpu.VMEM((tokens, width), half),
            pltpu.VMEM((tokens, width), half),
            pltpu.VMEM((window, width, 2 * lanes), half),
            pltpu.VMEM((3, width, lanes), half),
            pltpu.VMEM((window, 3, rows, lanes), jnp.float32),
            pltpu.VMEM((steps, 3, rows, lanes), half),
            pltpu.VMEM((steps, 3, rows, lanes), half),
            pltpu.VMEM((sends, 3, rows, lanes), half),
            pltpu.VMEM((sends, 3, rows, lanes), half),
            pltpu.VMEM((rows, 2 * lanes), half),
            pltpu.VMEM((2, rows, width), jnp.float32),
            pltpu.VMEM((tp - 1, rows, width), half),
            pltpu.VMEM((tp - 1, rows, width), half),
            dma((tp - 1,)), dma((tp - 1,)), dma((tp - 1,)), dma((tp - 1,)),
            dma((window, 2)), dma((3,)), dma((steps, 3, halves)), dma((steps, 3, halves)),
            dma((sends, 3, halves)), dma((sends, 3, halves)), dma((outs, 3)), dma((2,)),
            dma((tp - 1,)), dma((tp - 1,)),
        ],
        compiler_params=pltpu.CompilerParams(
            collective_id=0, has_side_effects=True, vmem_limit_bytes=VMEM_LIMIT
        ),
        name="line_sum",
    )(normed, cotangent, w_gate, w_up, w_down)


def grad_kernel(scale, *refs):
    lefts, grads, outs = refs[:2], refs[2:5], refs[5:]
    for left, grad, out in zip((lefts[0], lefts[0], lefts[1]), grads, outs):
        value = jnp.dot(left[...], grad[...], preferred_element_type=jnp.float32)
        out[0] = (value if scale == 1.0 else value * scale).astype(out.dtype)


def weight_grads(rows_t, cot_t, d_gate, d_up, hidden, scale):
    width, tokens = rows_t.shape
    hidden_units = d_gate.shape[1]
    block = next(size for size in (768, 256, 128) if hidden_units % size == 0)
    return pl.pallas_call(
        functools.partial(grad_kernel, scale),
        grid=(hidden_units // block,),
        out_shape=[jax.ShapeDtypeStruct((1, width, hidden_units), jnp.bfloat16)] * 3,
        in_specs=[pl.BlockSpec((width, tokens), lambda i: (0, 0))] * 2
        + [pl.BlockSpec((tokens, block), lambda i: (0, i))] * 3,
        out_specs=[pl.BlockSpec((1, width, block), lambda i: (0, 0, i))] * 3,
        compiler_params=pltpu.CompilerParams(
            dimension_semantics=("arbitrary",), vmem_limit_bytes=40 * 1024 * 1024
        ),
        cost_estimate=pl.CostEstimate(
            flops=6 * width * tokens * hidden_units,
            bytes_accessed=6 * hidden_units * (width + tokens),
            transcendentals=0,
        ),
        name="weight_grads",
    )(rows_t, cot_t, d_gate, d_up, hidden)


def local(normed, cotangent, w_gate, w_up, w_down):
    scale = 1.0 / math.sqrt(normed.shape[1] * lax.axis_size("tp"))
    exact = math.frexp(scale)[0] == 0.5
    hidden, d_gate, d_up, rows_t, cot_t, total = sum_and_activate(
        normed[0], cotangent[0], w_gate, w_up, w_down, scale if exact else 1.0
    )
    passed = shift(total[None], "section", 1)
    grads = weight_grads(rows_t, cot_t, d_gate, d_up, hidden, 1.0 if exact else scale)
    return (passed, *grads)


def solution(mesh):
    in_specs = (
        P("section", "tp", "fsdp"),
        P("section", "tp", "fsdp"),
        P("section", "fsdp", "tp"),
        P("section", "fsdp", "tp"),
        P("section", "fsdp", "tp"),
    )
    out_specs = (
        P("section", "tp", "fsdp"),
        P("section", "fsdp", "tp"),
        P("section", "fsdp", "tp"),
        P("section", "fsdp", "tp"),
    )
    return jax.shard_map(local, mesh=mesh, in_specs=in_specs, out_specs=out_specs, check_vma=False)
```
